256 devices in a mesh: seq: 64 (over z_lo, x, y), tp: 4 (over z_hi, core).
Axes of the slice: x: 4, y: 4, z: 8 (z_hi: 2, z_lo: 4; z = z_hi * 4 + z_lo), core: 2. Of those that a mesh axis runs over, the one named last changes fastest.
Arguments:
- states: bfloat16 [64, 128, 2048], P('seq', None, 'tp'), may hold values from -60 to 60, as said below
- cotangent: bfloat16 [64, 128, 2048], P('seq', None, 'tp'), may hold values from -12 to 12, as said below
- wq: bfloat16 [2048, 2048], P(None, 'tp'), may hold values from -0.125 to 0.125
- wk: bfloat16 [2048, 512], P(None, 'tp'), may hold values from -0.125 to 0.125
- wv: bfloat16 [2048, 512], P(None, 'tp'), may hold values from -0.125 to 0.125
- wo: bfloat16 [2048, 2048], P('tp'), may hold values from -0.125 to 0.125
Outputs:
- gram: float32 [64, 64], P('seq')
The draws below stay inside these ranges and needn't reach their ends.
Inputs may be any that keep to these rules, and one draw needn't show every extreme that they name: `states`: finite values. `cotangent`: finite values.
All inputs are finite; a program needn't handle non-finite values.
Results may differ from the reference program's by a relative error of at most 0.0025.
Values may be sent and summed in bfloat16 or wider, within the bound.
A program may use at most 64 MiB of HBM per device.

```python
import jax
import jax.numpy as jnp
from jax import lax

D = 2048
HEADS = 32
KV_HEADS = 8
HEAD_DIM = 64
TOKENS_PER_SEQ = 128
SEQUENCE_COUNT = 64


def candidate_rows(key):
    pick_key = jax.random.fold_in(key, 17)
    picked = jax.random.randint(pick_key, (SEQUENCE_COUNT, TOKENS_PER_SEQ), 0, 2).astype(jnp.int32)
    return picked + 2 * jnp.arange(TOKENS_PER_SEQ, dtype=jnp.int32)[None, :]


def draw_states(key, part):
    row_index = candidate_rows(key)
    table_key = jax.random.fold_in(key, 301)
    noise_key = jax.random.fold_in(key, 302)
    candidates = jax.random.normal(table_key, (2 * TOKENS_PER_SEQ, D), jnp.float32)
    noise = 0.4 * jax.random.normal(noise_key, (SEQUENCE_COUNT, TOKENS_PER_SEQ, D), jnp.float32)
    tokens_base = jnp.take(candidates, row_index, axis=0)
    return jnp.clip(tokens_base + noise, -12.0, 12.0).astype(jnp.bfloat16)


def draw_cotangent(key, part):
    row_index = candidate_rows(key)
    table_key = jax.random.fold_in(key, 401)
    noise_key = jax.random.fold_in(key, 402)
    candidates = jax.random.normal(table_key, (2 * TOKENS_PER_SEQ, D), jnp.float32)
    noise = 0.4 * jax.random.normal(noise_key, (SEQUENCE_COUNT, TOKENS_PER_SEQ, D), jnp.float32)
    tokens_base = jnp.take(candidates, row_index, axis=0)
    return jnp.clip(tokens_base + noise, -12.0, 12.0).astype(jnp.bfloat16)


def shard_levels(own_key, shape, cuts, low, high):
    def one(axis_at, parts):
        draws = jax.random.uniform(jax.random.fold_in(jax.random.fold_in(own_key, 6), axis_at), (parts,), jnp.float32, low / len(cuts), high / len(cuts))
        return jnp.repeat(jnp.exp(draws), shape[axis_at] // parts).reshape((-1,) + (1,) * (len(shape) - axis_at - 1))

    gain = one(*cuts[0])
    for cut in cuts[1:]:
        gain = gain * one(*cut)
    return gain


def centred(rng, extent, deviation, limit, shards=(), kind=jnp.bfloat16):
    drawn = deviation * jax.random.normal(rng, extent, jnp.float32)
    if shards:
        drawn = drawn * shard_levels(rng, extent, shards, -0.22, 0.18)
    return jnp.clip(drawn, -limit, limit).astype(kind)


def setup_inputs(seed: int = 0) -> dict:
    seeds = jax.random.split(jax.random.key(seed), 7)
    return {
        "states": draw_states(jax.random.fold_in(seeds[6], 71), 0),
        "cotangent": draw_cotangent(jax.random.fold_in(seeds[6], 71), 0),
        "wq": centred(seeds[2], (D, D), D ** -0.5, 0.125, ((1, 4),)),
        "wk": centred(seeds[3], (D, KV_HEADS * HEAD_DIM), D ** -0.5, 0.125, ((1, 4),)),
        "wv": centred(seeds[4], (D, KV_HEADS * HEAD_DIM), D ** -0.5, 0.125, ((1, 4),)),
        "wo": centred(seeds[5], (D, D), D ** -0.5, 0.125, ((0, 4),)),
    }


theta_base = 500000.0

def rope_tables(length, head_dim):
    half_dim = head_dim // 2
    freqs_k = theta_base ** (-(jnp.arange(half_dim, dtype=jnp.float32) * 2.0 / head_dim))
    angles = jnp.arange(length, dtype=jnp.float32)[:, None] * freqs_k[None, :]
    angles = jnp.concatenate([angles, angles], axis=1)
    return (jnp.cos(angles)[:, None, :], jnp.sin(angles)[:, None, :])

def rotate(values_in, cos_table, sine_table):
    half_dim = values_in.shape[-1] // 2
    turned = jnp.concatenate([-values_in[..., half_dim:], values_in[..., :half_dim]], axis=-1)
    return values_in * cos_table + turned * sine_table

def reference(states, cotangent, wq, wk, wv, wo):
    seqs, length, model_width = states.shape
    group_size = HEADS // KV_HEADS
    tok_rows = seqs * length
    cos_table, sine_table = rope_tables(length, HEAD_DIM)
    flat_states = states.reshape(tok_rows, model_width)
    query_heads = jnp.dot(flat_states, wq, preferred_element_type=jnp.float32).reshape(seqs, length, HEADS, HEAD_DIM)
    query_heads = rotate(query_heads, cos_table, sine_table).astype(jnp.bfloat16).reshape(seqs, length, KV_HEADS, group_size, HEAD_DIM)
    key_heads = jnp.dot(flat_states, wk, preferred_element_type=jnp.float32).reshape(seqs, length, KV_HEADS, HEAD_DIM)
    key_heads = rotate(key_heads, cos_table, sine_table).astype(jnp.bfloat16)
    value_heads = jnp.dot(flat_states, wv, preferred_element_type=jnp.float32).astype(jnp.bfloat16).reshape(seqs, length, KV_HEADS, HEAD_DIM)
    scores = jnp.einsum('sqkgd,stkd->skgqt', query_heads.astype(jnp.float32), key_heads.astype(jnp.float32)) * HEAD_DIM ** (-0.5)
    causal = jnp.arange(length)[:, None] >= jnp.arange(length)[None, :]
    scores = jnp.where(causal, scores, -jnp.inf)
    weights_bf = jax.nn.softmax(scores, axis=-1).astype(jnp.bfloat16)
    attended = jnp.einsum('skgqt,stkd->sqkgd', weights_bf.astype(jnp.float32), value_heads.astype(jnp.float32)).astype(jnp.bfloat16).reshape(seqs, length, model_width)
    grad_attended = lax.dot_general(cotangent.reshape(tok_rows, model_width), wo, (((1,), (1,)), ((), ())), preferred_element_type=jnp.float32).astype(jnp.bfloat16).reshape(seqs, length, KV_HEADS, group_size, HEAD_DIM)
    value_gradient = jnp.einsum('skgqt,sqkgd->stkd', weights_bf.astype(jnp.float32), grad_attended.astype(jnp.float32)).astype(jnp.bfloat16).reshape(seqs, length, KV_HEADS * HEAD_DIM)
    states_wide = states.astype(jnp.float32)
    grad_wv = jnp.einsum('std,stv->sdv', states_wide, value_gradient.astype(jnp.float32), precision=lax.Precision.HIGHEST)
    kernel = jnp.einsum('sdv,rdv->sr', grad_wv, grad_wv, precision=lax.Precision.HIGHEST)
    attended_wide = attended.astype(jnp.float32)
    cot_wide = cotangent.astype(jnp.float32)
    block_cols = model_width // 8

    def block_term(begin_col):
        cot_block = lax.dynamic_slice_in_dim(cot_wide, begin_col, block_cols, 2)
        grad_wo = jnp.einsum('std,ste->sde', attended_wide, cot_block, precision=lax.Precision.HIGHEST)
        return jnp.einsum('sde,rde->sr', grad_wo, grad_wo, precision=lax.Precision.HIGHEST)
    starts = (jnp.arange(8) * block_cols).astype(jnp.int32)
    kernel = kernel + lax.optimization_barrier(jnp.sum(lax.map(block_term, starts), axis=0))
    kernel_diag = jnp.diagonal(kernel)
    return kernel / jnp.sqrt(kernel_diag[:, None] * kernel_diag[None, :])
```

```python
import functools

import jax
import jax.numpy as jnp
import numpy as np
from jax import lax
from jax.experimental import pallas as pl
from jax.experimental.pallas import tpu as pltpu
from jax.sharding import Mesh
from jax.sharding import PartitionSpec as P

AXES = ("z", "x", "y", "h", "c")
MESH = pl.DeviceIdType.MESH
HEAD_DIM = 64
THETA = 500000.0
T = 128
PITCH = 72
BF = jnp.bfloat16
F32 = jnp.float32

PLANE = [(a, b) for a in range(4) for b in range(4) if (a, b) != (0, 0)]
COLUMN = [(w, c) for w in range(8) for c in range(2) if (w, c) != (0, 0)]


def nn(a, b):
    return lax.dot_general(a, b, (((1,), (0,)), ((), ())), preferred_element_type=F32)


def nt(a, b):
    return lax.dot_general(a, b, (((1,), (1,)), ((), ())), preferred_element_type=F32)


def rope_tables():
    k = np.arange(HEAD_DIM // 2, dtype=np.float64)
    freq = THETA ** (-2.0 * k / HEAD_DIM)
    angle = np.arange(T, dtype=np.float64)[:, None] * freq[None, :]
    cos, sin = np.cos(angle), np.sin(angle)
    cos = np.concatenate([cos, cos] * 2, axis=1)
    sin = np.concatenate([-sin, sin] * 2, axis=1)
    return cos.astype(np.float32), sin.astype(np.float32)


def rope(v, cos, sin):
    lane = lax.broadcasted_iota(jnp.int32, v.shape, 1)
    turned = jnp.where(lane % 64 < 32, pltpu.roll(v, 96, 1), pltpu.roll(v, 32, 1))
    return v * cos + turned * sin


def kernel(st, ct, wq, wk, wv, wo, cos, sin, out, wqb, wkb, wvb, wob, sbuf, cbuf, qacc, kacc, vacc,
           pst, a_own, v_own, abuf, vbuf, hsend, gsend, hbuf, gbuf, gram_in, kd, fin, f1, tbuf, f2,
           loc, tps, tpr, acs, acr, vcs, vcr, ccs, ccr, scs, scr, hs, hr, gs, gr, f1s, f1r, f2s, f2r):
    z, x, y, h, c = [lax.axis_index(a) for a in AXES]
    w = h * 4 + z
    p = h * 2 + c
    plane = x * 4 + y
    column = w * 2 + c
    other = 2 * (1 - h) + c

    def in_plane(a, b):
        return (z, (x + a) % 4, (y + b) % 4, h, c)

    def in_column(dw, dc):
        v = (w + dw) % 8
        return (v % 4, x, y, v // 4, (c + dc) % 2)

    sibling = in_column(0, 1)

    def remote(src, dst, send, recv, device):
        return pltpu.make_async_remote_copy(
            src_ref=src, dst_ref=dst, send_sem=send, recv_sem=recv, device_id=device, device_id_type=MESH)

    sent = []

    def push(src, dst, send, recv, device):
        copy = remote(src, dst, send, recv, device)
        copy.start()
        sent.append(copy)

    def arrived(slot, send, recv):
        remote(slot, slot, send, recv, sibling).wait_recv()

    loads = [pltpu.make_async_copy(a, b, loc.at[i]) for i, (a, b) in enumerate(
        [(st.at[0], sbuf.at[z, p]), (ct.at[0], cbuf.at[z, p]), (wq, wqb), (wk, wkb), (wv, wvb), (wo, wob)])]
    for load in loads:
        load.start()

    barrier = pltpu.get_barrier_semaphore()
    for a, b in PLANE:
        pl.semaphore_signal(barrier, inc=1, device_id=in_plane(a, b), device_id_type=MESH)
    for dw, dc in COLUMN:
        pl.semaphore_signal(barrier, inc=1, device_id=in_column(dw, dc), device_id_type=MESH)
    pl.semaphore_wait(barrier, len(PLANE) + len(COLUMN))

    loads[0].wait()
    push(sbuf.at[z, p], sbuf.at[z, p], tps.at[0], tpr.at[0], in_column(4, 0))
    push(sbuf.at[z, p], sbuf.at[z, p], tps.at[1], tpr.at[1], sibling)
    loads[1].wait()
    push(cbuf.at[z, p], cbuf.at[z, p], tps.at[2], tpr.at[2], in_column(4, 0))
    push(cbuf.at[z, p], cbuf.at[z, p], tps.at[3], tpr.at[3], sibling)

    def project(part, first):
        rows = pl.ds(pl.multiple_of(part * 512, 512), 512)
        s = sbuf[z, part]
        q, k, v = nn(s, wqb[rows, :]), nn(s, wkb[rows, :]), nn(s, wvb[rows, :])
        qacc[...] = q if first else qacc[...] + q
        kacc[...] = k if first else kacc[...] + k
        vacc[...] = v if first else vacc[...] + v

    for load in loads[2:5]:
        load.wait()
    project(p, True)
    arrived(sbuf.at[z, h * 2 + 1 - c], tps.at[1], tpr.at[1])
    project(h * 2 + 1 - c, False)
    arrived(sbuf.at[z, other], tps.at[0], tpr.at[0])
    push(sbuf.at[z, other], sbuf.at[z, other], tps.at[4], tpr.at[4], sibling)
    project(other, False)
    arrived(sbuf.at[z, 2 * (1 - h) + 1 - c], tps.at[4], tpr.at[4])
    project(2 * (1 - h) + 1 - c, False)

    cos_table, sin_table = cos[...], sin[...]
    lane = lax.broadcasted_iota(jnp.int32, (T, T), 1)
    key = rope(kacc[...], cos_table, sin_table)
    swapped = pltpu.roll(key, 64, 1)
    zero = jnp.zeros_like(key)
    low = lane < 64
    keys = [
        jnp.concatenate([jnp.where(low, key, zero), jnp.where(low, zero, swapped)], axis=0).astype(BF),
        jnp.concatenate([jnp.where(low, swapped, zero), jnp.where(low, zero, key)], axis=0).astype(BF),
    ]
    value_t = jnp.transpose(vacc[...]).astype(BF)
    row = lax.broadcasted_iota(jnp.int32, (T, T), 0)
    causal = row >= lane
    for j in range(4):
        query = rope(qacc[:, 128 * j : 128 * j + 128], cos_table, sin_table).astype(BF)
        scores = nt(query, keys[j // 2]) * HEAD_DIM ** (-0.5)
        for e in range(2):
            s = jnp.where(causal, scores[:, 128 * e : 128 * e + 128], -jnp.inf)
            s = jnp.exp(s - jnp.max(s, axis=1, keepdims=True))
            pst[2 * j + e] = (s / jnp.sum(s, axis=1, keepdims=True)).astype(BF)
    for g in range(2):
        probs = pst[4 * g : 4 * g + 4].reshape(4 * T, T)
        attended = nt(value_t[64 * g : 64 * g + 64], probs).astype(BF)
        for e in range(4):
            a_own[2 * g + e // 2, 64 * (e % 2) : 64 * (e % 2) + 64, :] = attended[:, 128 * e : 128 * e + 128]
    abuf[z, c] = a_own[z]
    push(abuf.at[z, c], abuf.at[z, c], acs.at[0], acr.at[0], sibling)
    for d in (1, 3, 2):
        to = (z + d) % 4
        push(a_own.at[to], abuf.at[z, c], acs.at[d], acr.at[d], (to, x, y, h, c))

    def gather(buf, send, recv):
        for i, (dw, parts) in enumerate([(1, (0, 1)), (7, (0, 1)), (2, (0,)), (6, (1,))]):
            for q in parts:
                part = 2 * q + c
                push(buf.at[z, part], buf.at[z, part], send.at[2 * i + q], recv.at[2 * i + q], in_column(dw, 0))

    def gathered(buf, send, recv, which):
        for i, back, parts in [(0, 3, (0, 1)), (1, 1, (0, 1)), (2, 2, (0,)), (3, 2, (1,))]:
            if back == which:
                for q in parts:
                    arrived(buf.at[(z + back) % 4, 2 * q + c], send.at[2 * i + q], recv.at[2 * i + q])

    arrived(cbuf.at[z, other], tps.at[2], tpr.at[2])
    push(cbuf.at[z, other], cbuf.at[z, other], tps.at[5], tpr.at[5], sibling)
    gather(cbuf, ccs, ccr)
    arrived(abuf.at[z, 1 - c], acs.at[0], acr.at[0])

    def forward_attended(d):
        came = (z - d) % 4
        arrived(abuf.at[came, c], acs.at[d], acr.at[d])
        push(abuf.at[came, c], abuf.at[came, c], acs.at[3 + d], acr.at[3 + d], sibling)

    def tiles(k, zz):
        left = abuf[zz].reshape(256, T)
        for q in range(2):
            block = nn(left, cbuf[zz, 2 * q + c]).astype(BF)
            for j in range(4):
                for e in range(2):
                    hsend[k, (4 * q + j) * 2 + e] = block[128 * e : 128 * e + 128, 128 * j : 128 * j + 128]
        hbuf[zz, plane] = hsend[k, plane]
        for i, (a, b) in enumerate(PLANE):
            to = (x + a) % 4 * 4 + (y + b) % 4
            push(hsend.at[k, to], hbuf.at[zz, plane], hs.at[k, i], hr.at[k, i], in_plane(a, b))

    tiles(0, z)

    loads[5].wait()
    arrived(cbuf.at[z, h * 2 + 1 - c], tps.at[3], tpr.at[3])
    arrived(cbuf.at[z, 2 * (1 - h) + 1 - c], tps.at[5], tpr.at[5])
    grad_t = nt(wob[:, 0:512], cbuf[z, 0])
    for part in range(1, 4):
        grad_t += nt(wob[:, 512 * part : 512 * part + 512], cbuf[z, part])
    grad_t = grad_t.astype(BF)
    for g in range(2):
        left = jnp.concatenate([grad_t[64 * (4 * g + e) : 64 * (4 * g + e) + 64] for e in range(4)], axis=1)
        gv = nn(left, pst[4 * g : 4 * g + 4].reshape(4 * T, T)).astype(BF)
        v_own[2 * g], v_own[2 * g + 1] = gv[0:32], gv[32:64]
    vbuf[z, c] = v_own[z]
    push(vbuf.at[z, c], vbuf.at[z, c], vcs.at[0], vcr.at[0], sibling)
    for d in (1, 3, 2):
        to = (z + d) % 4
        push(v_own.at[to], vbuf.at[z, c], vcs.at[d], vcr.at[d], (to, x, y, h, c))
    gather(sbuf, scs, scr)
    for d in (1, 3, 2):
        forward_attended(d)

    def settle(k, zz):
        def take(src, carry):
            gram_in[pl.ds(zz * 16 + src, 128, stride=PITCH), :] = hbuf[zz, src].astype(F32)
            return carry

        for i, (a, b) in enumerate(PLANE):
            src = (x - a) % 4 * 4 + (y - b) % 4
            arrived(hbuf.at[zz, src], hs.at[k, i], hr.at[k, i])
        lax.fori_loop(0, 16, take, 0)

    order = [0, 1, 3, 2]
    for k in range(1, 4):
        d = order[k]
        zz = (z + d) % 4
        arrived(abuf.at[zz, 1 - c], acs.at[3 + (4 - d) % 4], acr.at[3 + (4 - d) % 4])
        gathered(cbuf, ccs, ccr, d)
        tiles(k, zz)
        settle(k - 1, (z + order[k - 1]) % 4)

    for d in (1, 3, 2):
        came = (z - d) % 4
        arrived(vbuf.at[came, c], vcs.at[d], vcr.at[d])
        push(vbuf.at[came, c], vbuf.at[came, c], vcs.at[3 + d], vcr.at[3 + d], sibling)
    arrived(vbuf.at[z, 1 - c], vcs.at[0], vcr.at[0])
    for k in range(4):
        d = order[k]
        zz = (z + d) % 4
        if k > 0:
            arrived(vbuf.at[zz, 1 - c], vcs.at[3 + (4 - d) % 4], vcr.at[3 + (4 - d) % 4])
            gathered(sbuf, scs, scr, d)
        left = vbuf[zz].reshape(64, T)
        for q in range(2):
            block = nn(left, sbuf[zz, 2 * q + c]).astype(BF)
            for j in range(4):
                for e in range(2):
                    gsend[(4 * q + j) * 2 + e, zz] = block[32 * e : 32 * e + 32, 128 * j : 128 * j + 128]
    gbuf[plane] = gsend[plane]
    for i, (a, b) in enumerate(PLANE):
        to = (x + a) % 4 * 4 + (y + b) % 4
        push(gsend.at[to], gbuf.at[plane], gs.at[i], gr.at[i], in_plane(a, b))
    settle(3, (z + order[3]) % 4)
    for i, (a, b) in enumerate(PLANE):
        src = (x - a) % 4 * 4 + (y - b) % 4
        arrived(gbuf.at[src], gs.at[i], gr.at[i])

    def take_values(src, carry):
        for zz in range(4):
            gram_in[pl.ds(128 * PITCH + zz * 16 + src, 32, stride=PITCH), :] = gbuf[src, zz].astype(F32)
        return carry

    lax.fori_loop(0, 16, take_values, 0)

    def products(r, total):
        for u in range(4):
            at = pl.multiple_of((r * 8 + 2 * u) * PITCH, 8)
            both = jnp.concatenate([gram_in[pl.ds(at, 64), :], gram_in[pl.ds(at + PITCH, 64), :]], axis=1).astype(BF)
            total = total + nt(both, both)
        return total

    share = lax.fori_loop(0, 20, products, jnp.zeros((64, 64), F32))
    eye = lax.broadcasted_iota(jnp.int32, (64, 64), 0) == lax.broadcasted_iota(jnp.int32, (64, 64), 1)
    diag = jnp.sum(jnp.where(eye, share, 0.0), axis=0, keepdims=True)
    kd[...] = jnp.concatenate([share, jnp.broadcast_to(diag, (64, 64))], axis=1)
    for g in range(16):
        fin[g] = kd[pl.ds(g, 4, stride=16), :]
    f1[plane] = fin[plane]
    for i, (a, b) in enumerate(PLANE):
        to = (x + a) % 4 * 4 + (y + b) % 4
        push(fin.at[to], f1.at[plane], f1s.at[i], f1r.at[i], in_plane(a, b))
    for i, (a, b) in enumerate(PLANE):
        src = (x - a) % 4 * 4 + (y - b) % 4
        arrived(f1.at[src], f1s.at[i], f1r.at[i])
    rows = jnp.sum(f1[...], axis=0)
    for zz in range(4):
        tbuf[zz] = rows[zz : zz + 1]
    f2[column] = tbuf[z]
    for i, (dw, dc) in enumerate(COLUMN):
        to = in_column(dw, dc)
        push(tbuf.at[to[0]], f2.at[column], f2s.at[i], f2r.at[i], to)
    for i, (dw, dc) in enumerate(COLUMN):
        src = (w - dw) % 8 * 2 + (c - dc) % 2
        arrived(f2.at[src], f2s.at[i], f2r.at[i])
    total = jnp.sum(f2[...], axis=0)
    entries, diagonal = total[:, 0:64], total[:, 64:128]
    mine = lax.broadcasted_iota(jnp.int32, (1, 64), 1) == z * 16 + plane
    own = jnp.sum(jnp.where(mine, diagonal, 0.0), axis=1, keepdims=True)
    out[...] = entries / jnp.sqrt(own * diagonal)
    for copy in sent:
        copy.wait_send()


def on_device(states, cotangent, wq, wk, wv, wo):
    cos, sin = rope_tables()
    any_spec = pl.BlockSpec(memory_space=pl.ANY)
    vmem = pl.BlockSpec(memory_space=pltpu.VMEM)
    dma = pltpu.SemaphoreType.DMA
    shapes = [
        ((2048, 512), BF), ((2048, 128), BF), ((2048, 128), BF), ((512, 2048), BF),
        ((4, 4, T, 512), BF), ((4, 4, T, 512), BF),
        ((T, 512), F32), ((T, 128), F32), ((T, 128), F32),
        ((8, T, T), BF), ((4, 128, T), BF), ((4, 32, T), BF), ((4, 2, 128, T), BF), ((4, 2, 32, T), BF),
        ((4, 16, 128, 128), BF), ((16, 4, 32, 128), BF), ((4, 16, 128, 128), BF), ((16, 4, 32, 128), BF),
        ((160 * PITCH, 128), F32), ((64, 128), F32), ((16, 4, 128), F32), ((16, 4, 128), F32),
        ((4, 1, 128), F32), ((16, 1, 128), F32),
    ]
    sems = [(6,), (6,), (6,), (7,), (7,), (7,), (7,), (8,), (8,), (8,), (8,), (4, 15), (4, 15), (15,), (15,), (15,), (15,), (15,), (15,)]
    return pl.pallas_call(
        kernel,
        out_shape=jax.ShapeDtypeStruct((1, 64), F32),
        in_specs=[any_spec] * 6 + [vmem] * 2,
        out_specs=vmem,
        scratch_shapes=[pltpu.VMEM(s, t) for s, t in shapes] + [dma(s) for s in sems],
        compiler_params=pltpu.CompilerParams(
            collective_id=0, has_side_effects=True, vmem_limit_bytes=60 * 2**20),
        name="ntk_gram",
    )(states, cotangent, wq, wk, wv, wo, jnp.asarray(cos), jnp.asarray(sin))


def solution(mesh):
    split = Mesh(mesh.devices.reshape(4, 4, 4, 2, 2), AXES)
    seq, tp = ("z", "x", "y"), ("h", "c")
    return jax.shard_map(
        on_device,
        mesh=split,
        in_specs=(P(seq, None, tp), P(seq, None, tp), P(None, tp), P(None, tp), P(None, tp), P(tp, None)),
        out_specs=P(seq, None),
        check_vma=False,
    )
```

```python
import functools

import jax
import jax.numpy as jnp
import numpy as np
from jax import lax
from jax.experimental import pallas as pl
from jax.experimental.pallas import tpu as pltpu
from jax.sharding import Mesh
from jax.sharding import PartitionSpec as P

AXES = ("z", "x", "y", "h", "c")
MESH = pl.DeviceIdType.MESH
HEAD_DIM = 64
THETA = 500000.0
T = 128
PITCH = 72
BF = jnp.bfloat16
F32 = jnp.float32

PLANE = [(2, 2), (2, 1), (1, 2), (2, 3), (3, 2), (1, 1), (3, 3), (1, 3), (3, 1), (2, 0), (0, 2), (1, 0), (3, 0), (0, 1), (0, 3)]
COLUMN = [(w, c) for w in range(8) for c in range(2) if (w, c) != (0, 0)]


def nn(a, b):
    return lax.dot_general(a, b, (((1,), (0,)), ((), ())), preferred_element_type=F32)


def nt(a, b):
    return lax.dot_general(a, b, (((1,), (1,)), ((), ())), preferred_element_type=F32)


def rope_tables():
    k = np.arange(HEAD_DIM // 2, dtype=np.float64)
    freq = THETA ** (-2.0 * k / HEAD_DIM)
    angle = np.arange(T, dtype=np.float64)[:, None] * freq[None, :]
    cos, sin = np.cos(angle), np.sin(angle)
    cos = np.concatenate([cos, cos] * 2, axis=1)
    sin = np.concatenate([-sin, sin] * 2, axis=1)
    return cos.astype(np.float32), sin.astype(np.float32)


def rope(v, cos, sin):
    lane = lax.broadcasted_iota(jnp.int32, v.shape, 1)
    turned = jnp.where(lane % 64 < 32, pltpu.roll(v, 96, 1), pltpu.roll(v, 32, 1))
    return v * cos + turned * sin


def kernel(st, ct, wq, wk, wv, wo, cos_in, sin_in, out, wqb, wkb, wvb, wob, cos, sin, sbuf, cbuf, sq, cq, qacc, kacc, vacc,
           pst, abuf, vbuf, tsend, tbuf, gram_in, kd, fin, f1, rowbuf, f2,
           loc, tps, tpr, acs, acr, vcs, vcr, ccs, ccr, scs, scr, hs, hr, gs, gr, f1s, f1r, f2s, f2r):
    z, x, y, h, c = [lax.axis_index(a) for a in AXES]
    w = h * 4 + z
    p = h * 2 + c
    plane = x * 4 + y
    column = w * 2 + c

    def in_plane(a, b):
        return (z, (x + a) % 4, (y + b) % 4, h, c)

    def in_column(dw, dc):
        v = (w + dw) % 8
        return (v % 4, x, y, v // 4, (c + dc) % 2)

    sibling = in_column(0, 1)
    opposite = in_column(4, 0)

    def remote(src, dst, send, recv, device):
        return pltpu.make_async_remote_copy(
            src_ref=src, dst_ref=dst, send_sem=send, recv_sem=recv, device_id=device, device_id_type=MESH)

    sent = []

    def push(src, dst, send, recv, device):
        copy = remote(src, dst, send, recv, device)
        copy.start()
        sent.append(copy)

    def arrived(slot, send, recv):
        remote(slot, slot, send, recv, sibling).wait_recv()

    loads = [pltpu.make_async_copy(a, b, loc.at[i]) for i, (a, b) in enumerate(
        [(st.at[0], sbuf.at[p]), (ct.at[0], cbuf.at[p]), (wq, wqb), (wk, wkb), (wv, wvb), (cos_in, cos), (sin_in, sin), (wo, wob)])]
    for load in loads:
        load.start()

    barrier = pltpu.get_barrier_semaphore()
    for dw, dc in COLUMN:
        pl.semaphore_signal(barrier, inc=1, device_id=in_column(dw, dc), device_id_type=MESH)
    for a, b in PLANE:
        pl.semaphore_signal(barrier, inc=1, device_id=in_plane(a, b), device_id_type=MESH)
    pl.semaphore_wait(barrier, len(PLANE) + len(COLUMN))

    halves = [pl.ds(0, 256), pl.ds(256, 256)]

    def exchange(buf, base):
        for i, cols in enumerate(halves):
            push(buf.at[p, :, cols], buf.at[p, :, cols], tps.at[base + i], tpr.at[base + i], opposite)
        push(buf.at[p], buf.at[p], tps.at[base + 2], tpr.at[base + 2], sibling)

    def from_sibling(buf, base):
        arrived(buf.at[h * 2 + 1 - c], tps.at[base + 2], tpr.at[base + 2])

    def from_opposite(buf, base, i):
        part = buf.at[2 * (1 - h) + c, :, halves[i]]
        arrived(part, tps.at[base + i], tpr.at[base + i])
        push(part, part, tps.at[base + 3 + i], tpr.at[base + 3 + i], sibling)

    def forwarded(buf, base, i):
        arrived(buf.at[2 * (1 - h) + 1 - c, :, halves[i]], tps.at[base + 3 + i], tpr.at[base + 3 + i])

    loads[0].wait()
    exchange(sbuf, 0)
    loads[1].wait()
    exchange(cbuf, 5)
    def project(part, i, width, first=False):
        rows = pl.ds(pl.multiple_of(part * 512 + 256 * i, 256), width)
        s = sbuf[part, :, 256 * i : 256 * i + width]
        q, k, v = nn(s, wqb[rows, :]), nn(s, wkb[rows, :]), nn(s, wvb[rows, :])
        qacc[...] = q if first else qacc[...] + q
        kacc[...] = k if first else kacc[...] + k
        vacc[...] = v if first else vacc[...] + v

    for load in loads[2:7]:
        load.wait()
    project(p, 0, 512, True)
    from_sibling(sbuf, 0)
    project(h * 2 + 1 - c, 0, 512)
    cos_table, sin_table = cos[...], sin[...]
    for i in range(2):
        from_opposite(sbuf, 0, i)
        project(2 * (1 - h) + c, i, 256)
    for i in range(2):
        forwarded(sbuf, 0, i)
        project(2 * (1 - h) + 1 - c, i, 256)

    lane = lax.broadcasted_iota(jnp.int32, (T, T), 1)
    key = rope(kacc[...], cos_table, sin_table)
    swapped = pltpu.roll(key, 64, 1)
    zero = jnp.zeros_like(key)
    low = lane < 64
    keys = [
        jnp.concatenate([jnp.where(low, key, zero), jnp.where(low, zero, swapped)], axis=0).astype(BF),
        jnp.concatenate([jnp.where(low, swapped, zero), jnp.where(low, zero, key)], axis=0).astype(BF),
    ]
    value_t = jnp.transpose(vacc[...]).astype(BF)
    row = lax.broadcasted_iota(jnp.int32, (T, T), 0)
    causal = row >= lane
    for j in range(4):
        query = rope(qacc[:, 128 * j : 128 * j + 128], cos_table, sin_table).astype(BF)
        scores = nt(query, keys[j // 2]) * HEAD_DIM ** (-0.5)
        for e in range(2):
            s = jnp.where(causal, scores[:, 128 * e : 128 * e + 128], -jnp.inf)
            s = jnp.exp(s - jnp.max(s, axis=1, keepdims=True))
            pst[2 * j + e] = (s / jnp.sum(s, axis=1, keepdims=True)).astype(BF)
    for g in range(2):
        probs = pst[4 * g : 4 * g + 4].reshape(4 * T, T)
        attended = nt(value_t[64 * g : 64 * g + 64], probs).astype(BF)
        for e in range(4):
            r = 64 * (4 * g + e)
            abuf[z, r : r + 64, :] = attended[:, 128 * e : 128 * e + 128]

    def along_z(buf, send, recv, k):
        push(buf.at[z], buf.at[z], send.at[k], recv.at[k], (z ^ k, x, y, h, c))

    along_z(abuf, acs, acr, 1)

    mine = pl.ds(pl.multiple_of(64 * c, 64), 64)
    others = pl.ds(pl.multiple_of(64 * (1 - c), 64), 64)

    def quarter(buf, kept, send, recv, i, dw):
        push(buf.at[(z + dw) % 4, mine, :], kept.at[z, mine, :], send.at[i], recv.at[i], in_column(dw, 0))

    def relay(kept, send, recv, k):
        i = 2 if k == 2 else (1 - z % 2 if k == 1 else z % 2)
        arrived(kept.at[z ^ k, mine, :], send.at[i], recv.at[i])
        push(kept.at[z ^ k, mine, :], kept.at[z ^ k, mine, :], send.at[2 + k], recv.at[2 + k], sibling)

    def complete(kept, send, recv, k):
        arrived(kept.at[z ^ k, others, :], send.at[2 + k], recv.at[2 + k])

    from_sibling(cbuf, 5)
    from_opposite(cbuf, 5, 0)
    from_opposite(cbuf, 5, 1)
    forwarded(cbuf, 5, 0)
    forwarded(cbuf, 5, 1)
    quarter(cbuf, cq, ccs, ccr, 0, 1)
    quarter(cbuf, cq, ccs, ccr, 1, 7)
    quarter(cbuf, cq, ccs, ccr, 2, 6)
    along_z(abuf, acs, acr, 3)

    def tile_wo(k, right):
        for rb in range(4):
            block = nn(abuf[z ^ k, 128 * rb : 128 * rb + 128, :], right).astype(BF)
            for cb in range(4):
                tsend[k, rb * 4 + cb, 0:128, :] = block[:, 128 * cb : 128 * cb + 128]
        tbuf[z ^ k, plane, 0:128, :] = tsend[k, plane, 0:128, :]
        for i, (a, b) in enumerate(PLANE):
            to = (x + a) % 4 * 4 + (y + b) % 4
            push(tsend.at[k, to, pl.ds(0, 128)], tbuf.at[z ^ k, plane, pl.ds(0, 128)], hs.at[k, i], hr.at[k, i], in_plane(a, b))

    def tile_wv(k, right):
        block = nn(vbuf[z ^ k], right).astype(BF)
        for rb in range(4):
            for cb in range(4):
                tsend[k, rb * 4 + cb, 128:160, :] = block[32 * rb : 32 * rb + 32, 128 * cb : 128 * cb + 128]
        tbuf[z ^ k, plane, 128:160, :] = tsend[k, plane, 128:160, :]
        for i, (a, b) in enumerate(PLANE):
            to = (x + a) % 4 * 4 + (y + b) % 4
            push(tsend.at[k, to, pl.ds(128, 32)], tbuf.at[z ^ k, plane, pl.ds(128, 32)], gs.at[k, i], gr.at[k, i], in_plane(a, b))

    tile_wo(0, cbuf[z])
    along_z(abuf, acs, acr, 2)
    quarter(sbuf, sq, scs, scr, 0, 1)
    quarter(sbuf, sq, scs, scr, 1, 7)

    loads[7].wait()
    grad_t = nt(wob[:, 0:512], cbuf[0])
    for part in range(1, 4):
        grad_t += nt(wob[:, 512 * part : 512 * part + 512], cbuf[part])
    grad_t = grad_t.astype(BF)
    for g in range(2):
        left = jnp.concatenate([grad_t[64 * (4 * g + e) : 64 * (4 * g + e) + 64] for e in range(4)], axis=1)
        vbuf[z, 64 * g : 64 * g + 64, :] = nn(left, pst[4 * g : 4 * g + 4].reshape(4 * T, T)).astype(BF)
    along_z(vbuf, vcs, vcr, 1)
    along_z(vbuf, vcs, vcr, 3)
    quarter(sbuf, sq, scs, scr, 2, 2)
    along_z(vbuf, vcs, vcr, 2)
    tile_wv(0, sbuf[z])
    gram_in[...] = jnp.zeros_like(gram_in)

    def settle_wo(k):
        def take(src, carry):
            gram_in[pl.ds((z ^ k) * 16 + src, 128, stride=PITCH), :] = tbuf[z ^ k, src, 0:128, :].astype(F32)
            return carry

        for i, (a, b) in enumerate(PLANE):
            src = (x - a) % 4 * 4 + (y - b) % 4
            arrived(tbuf.at[z ^ k, src, pl.ds(0, 128)], hs.at[k, i], hr.at[k, i])
        lax.fori_loop(0, 16, take, 0)

    def settle_wv(k):
        def take(src, carry):
            gram_in[pl.ds(128 * PITCH + (z ^ k) * 16 + src, 32, stride=PITCH), :] = tbuf[z ^ k, src, 128:160, :].astype(F32)
            return carry

        for i, (a, b) in enumerate(PLANE):
            src = (x - a) % 4 * 4 + (y - b) % 4
            arrived(tbuf.at[z ^ k, src, pl.ds(128, 32)], gs.at[k, i], gr.at[k, i])
        lax.fori_loop(0, 16, take, 0)

    def next_wo(k):
        arrived(abuf.at[z ^ k], acs.at[k], acr.at[k])
        complete(cq, ccs, ccr, k)
        tile_wo(k, cq[z ^ k])

    def next_wv(k):
        arrived(vbuf.at[z ^ k], vcs.at[k], vcr.at[k])
        complete(sq, scs, scr, k)
        tile_wv(k, sq[z ^ k])

    relay(cq, ccs, ccr, 1)
    relay(cq, ccs, ccr, 3)
    next_wo(1)
    relay(cq, ccs, ccr, 2)
    next_wo(3)
    relay(sq, scs, scr, 1)
    relay(sq, scs, scr, 3)
    next_wv(1)
    next_wo(2)
    relay(sq, scs, scr, 2)
    next_wv(3)
    next_wv(2)
    def pair(r, u, first, size):
        at = (r * 32 + 2 * u) * PITCH + first
        upper = gram_in[pl.ds(pl.multiple_of(at, 8), size), :]
        lower = gram_in[pl.ds(pl.multiple_of(at + PITCH, 8), size), :]
        return jnp.concatenate([upper, lower], axis=1).astype(BF)

    def products(r, total):
        for u in range(16):
            both = pair(r, u, 0, 64)
            total = total + nt(both, both)
        return total

    late = (z ^ 2) * 16

    def late_products(r, total):
        for u in range(16):
            total = total + nt(pair(r, u, 0, 64), pair(r, u, late, 16))
        return total

    for k in (0, 1, 3):
        settle_wo(k)
    kd[:, 0:64] = lax.fori_loop(0, 4, products, jnp.zeros((64, 64), F32))
    settle_wv(0)
    settle_wv(1)
    settle_wo(2)
    strip = lax.fori_loop(0, 4, late_products, jnp.zeros((64, 16), F32))
    wide = jnp.concatenate([strip, jnp.zeros((64, 112), F32)], axis=1)
    wide = pltpu.roll(wide, late, 1)[:, 0:64]
    lanes = lax.broadcasted_iota(jnp.int32, (64, 64), 1)
    kd[:, 0:64] = jnp.where((lanes >= late) & (lanes < late + 16), wide, kd[:, 0:64])
    kd[pl.ds(pl.multiple_of(late, 16), 16), 0:64] = jnp.transpose(strip)
    settle_wv(3)
    settle_wv(2)
    kd[:, 0:64] = products(4, kd[:, 0:64])
    eye = lax.broadcasted_iota(jnp.int32, (64, 64), 0) == lanes
    diag = jnp.sum(jnp.where(eye, kd[:, 0:64], 0.0), axis=0, keepdims=True)
    kd[:, 64:128] = jnp.broadcast_to(diag, (64, 64))
    for g in range(16):
        fin[g] = kd[pl.ds(g, 4, stride=16), :]
    f1[plane] = fin[plane]
    for i, (a, b) in enumerate(PLANE):
        to = (x + a) % 4 * 4 + (y + b) % 4
        push(fin.at[to], f1.at[plane], f1s.at[i], f1r.at[i], in_plane(a, b))
    for i, (a, b) in enumerate(PLANE):
        src = (x - a) % 4 * 4 + (y - b) % 4
        arrived(f1.at[src], f1s.at[i], f1r.at[i])
    rows = jnp.sum(f1[...], axis=0)
    for zz in range(4):
        rowbuf[zz] = rows[zz : zz + 1]
    f2[column] = rowbuf[z]
    for i, (dw, dc) in enumerate(COLUMN):
        to = in_column(dw, dc)
        push(rowbuf.at[to[0]], f2.at[column], f2s.at[i], f2r.at[i], to)
    for i, (dw, dc) in enumerate(COLUMN):
        src = (w - dw) % 8 * 2 + (c - dc) % 2
        arrived(f2.at[src], f2s.at[i], f2r.at[i])
    total = jnp.sum(f2[...], axis=0)
    entries, diagonal = total[:, 0:64], total[:, 64:128]
    own_lane = lax.broadcasted_iota(jnp.int32, (1, 64), 1) == z * 16 + plane
    own = jnp.sum(jnp.where(own_lane, diagonal, 0.0), axis=1, keepdims=True)
    out[...] = entries / jnp.sqrt(own * diagonal)
    for copy in sent:
        copy.wait_send()


def on_device(states, cotangent, wq, wk, wv, wo):
    cos, sin = rope_tables()
    any_spec = pl.BlockSpec(memory_space=pl.ANY)
    dma = pltpu.SemaphoreType.DMA
    shapes = [
        ((2048, 512), BF), ((2048, 128), BF), ((2048, 128), BF), ((512, 2048), BF), ((T, T), F32), ((T, T), F32),
        ((4, T, 512), BF), ((4, T, 512), BF), ((4, T, 512), BF), ((4, T, 512), BF),
        ((T, 512), F32), ((T, 128), F32), ((T, 128), F32),
        ((8, T, T), BF), ((4, 512, T), BF), ((4, 128, T), BF),
        ((4, 16, 160, 128), BF), ((4, 16, 160, 128), BF),
        ((160 * PITCH, 128), F32), ((64, 128), F32), ((16, 4, 128), F32), ((16, 4, 128), F32),
        ((4, 1, 128), F32), ((16, 1, 128), F32),
    ]
    sems = [(8,)] + [(10,)] * 2 + [(4,)] * 4 + [(6,)] * 4 + [(4, 15)] * 4 + [(15,)] * 4
    return pl.pallas_call(
        kernel,
        out_shape=jax.ShapeDtypeStruct((1, 64), F32),
        in_specs=[any_spec] * 8,
        out_specs=pl.BlockSpec(memory_space=pltpu.VMEM),
        scratch_shapes=[pltpu.VMEM(s, t) for s, t in shapes] + [dma(s) for s in sems],
        compiler_params=pltpu.CompilerParams(
            collective_id=0, has_side_effects=True, vmem_limit_bytes=60 * 2**20),
        name="ntk_gram",
    )(states, cotangent, wq, wk, wv, wo, jnp.asarray(cos), jnp.asarray(sin))


def solution(mesh):
    split = Mesh(mesh.devices.reshape(4, 4, 4, 2, 2), AXES)
    seq, tp = ("z", "x", "y"), ("h", "c")
    return jax.shard_map(
        on_device,
        mesh=split,
        in_specs=(P(seq, None, tp), P(seq, None, tp), P(None, tp), P(None, tp), P(None, tp), P(tp, None)),
        out_specs=P(seq, None),
        check_vma=False,
    )
```

```python
import functools

import jax
import jax.numpy as jnp
import numpy as np
from jax import lax
from jax.experimental import pallas as pl
from jax.experimental.pallas import tpu as pltpu
from jax.sharding import Mesh
from jax.sharding import PartitionSpec as P

AXES = ("z", "x", "y", "h", "c")
MESH = pl.DeviceIdType.MESH
HEAD_DIM = 64
THETA = 500000.0
T = 128
PITCH = 72
BF = jnp.bfloat16
F32 = jnp.float32

PLANE = [(2, 2), (2, 1), (1, 2), (2, 3), (3, 2), (1, 1), (3, 3), (1, 3), (3, 1), (2, 0), (0, 2), (1, 0), (3, 0), (0, 1), (0, 3)]
COLUMN = [(w, c) for w in range(8) for c in range(2) if (w, c) != (0, 0)]


def nn(a, b):
    return lax.dot_general(a, b, (((1,), (0,)), ((), ())), preferred_element_type=F32)


def nt(a, b):
    return lax.dot_general(a, b, (((1,), (1,)), ((), ())), preferred_element_type=F32)


def rope_tables():
    k = np.arange(HEAD_DIM // 2, dtype=np.float64)
    freq = THETA ** (-2.0 * k / HEAD_DIM)
    angle = np.arange(T, dtype=np.float64)[:, None] * freq[None, :]
    cos, sin = np.cos(angle), np.sin(angle)
    cos = np.concatenate([cos, cos] * 2, axis=1)
    sin = np.concatenate([-sin, sin] * 2, axis=1)
    return cos.astype(np.float32), sin.astype(np.float32)


def rope(v, cos, sin):
    lane = lax.broadcasted_iota(jnp.int32, v.shape, 1)
    turned = jnp.where(lane % 64 < 32, pltpu.roll(v, 96, 1), pltpu.roll(v, 32, 1))
    return v * cos + turned * sin


def kernel(st, ct, wq, wk, wv, wo, cos_in, sin_in, out, wqb, wkb, wvb, wob, cos, sin, sbuf, cbuf, sq, cq, qacc, kacc, vacc, gacc,
           pst, abuf, vbuf, tsend, tbuf, gram_in, kd, fin, f1, rowbuf, f2,
           loc, tps, tpr, acs, acr, vcs, vcr, ccs, ccr, scs, scr, hs, hr, gs, gr, f1s, f1r, f2s, f2r):
    z, x, y, h, c = [lax.axis_index(a) for a in AXES]
    w = h * 4 + z
    p = h * 2 + c
    plane = x * 4 + y
    column = w * 2 + c

    def in_plane(a, b):
        return (z, (x + a) % 4, (y + b) % 4, h, c)

    def in_column(dw, dc):
        v = (w + dw) % 8
        return (v % 4, x, y, v // 4, (c + dc) % 2)

    sibling = in_column(0, 1)
    opposite = in_column(4, 0)

    def remote(src, dst, send, recv, device):
        return pltpu.make_async_remote_copy(
            src_ref=src, dst_ref=dst, send_sem=send, recv_sem=recv, device_id=device, device_id_type=MESH)

    sent = []

    def push(src, dst, send, recv, device):
        copy = remote(src, dst, send, recv, device)
        copy.start()
        sent.append(copy)

    def arrived(slot, send, recv):
        remote(slot, slot, send, recv, sibling).wait_recv()

    barrier = pltpu.get_barrier_semaphore()
    for dw, dc in COLUMN:
        pl.semaphore_signal(barrier, inc=1, device_id=in_column(dw, dc), device_id_type=MESH)
    for a, b in PLANE:
        pl.semaphore_signal(barrier, inc=1, device_id=in_plane(a, b), device_id_type=MESH)
    loads = [pltpu.make_async_copy(a, b, loc.at[i]) for i, (a, b) in enumerate(
        [(st.at[0], sbuf.at[p]), (ct.at[0], cbuf.at[p]), (wq, wqb), (wk, wkb), (wv, wvb), (cos_in, cos), (sin_in, sin), (wo, wob)])]
    for load in loads:
        load.start()
    pl.semaphore_wait(barrier, len(PLANE) + len(COLUMN))

    halves = [pl.ds(0, 256), pl.ds(256, 256)]

    def to_opposite(buf, base):
        for i, cols in enumerate(halves):
            push(buf.at[p, :, cols], buf.at[p, :, cols], tps.at[base + i], tpr.at[base + i], opposite)

    def to_sibling(buf, base):
        push(buf.at[p], buf.at[p], tps.at[base + 2], tpr.at[base + 2], sibling)

    near = (h == z // 2)
    strips = [pl.ds(0, 64), pl.ds(64, 64)]

    def spread(t, which, core):
        rows = strips[core]
        return remote(cbuf.at[p, rows, :], cq.at[z, rows, :], ccs.at[2 * which + core], ccr.at[z], (p, x, y, t, core))

    kept_here = 2 * (1 - h) + c == z
    kept_there = 2 * (1 - h) + 1 - c == z

    def cot_half(part, i, at, device):
        cols = halves[i]
        return remote(cbuf.at[part, :, cols], cbuf.at[part, :, cols], tps.at[at + i], tpr.at[at + i], device)

    def from_sibling(buf, base):
        arrived(buf.at[h * 2 + 1 - c], tps.at[base + 2], tpr.at[base + 2])

    def from_opposite(buf, base, i):
        part = buf.at[2 * (1 - h) + c, :, halves[i]]
        arrived(part, tps.at[base + i], tpr.at[base + i])
        push(part, part, tps.at[base + 3 + i], tpr.at[base + 3 + i], sibling)

    def forwarded(buf, base, i):
        arrived(buf.at[2 * (1 - h) + 1 - c, :, halves[i]], tps.at[base + 3 + i], tpr.at[base + 3 + i])

    loads[0].wait()
    to_opposite(sbuf, 0)
    to_sibling(sbuf, 0)
    loads[1].wait()
    to_sibling(cbuf, 5)
    for core in range(2):
        spread(1 - h, 0, core).start()

    @pl.when(z != p)
    def _():
        for core in range(2):
            spread(h, 1, core).start()

    def project(part, i, width, first=False):
        rows = pl.ds(pl.multiple_of(part * 512 + 256 * i, 256), width)
        s = sbuf[part, :, 256 * i : 256 * i + width]
        q, k, v = nn(s, wqb[rows, :]), nn(s, wkb[rows, :]), nn(s, wvb[rows, :])
        qacc[...] = q if first else qacc[...] + q
        kacc[...] = k if first else kacc[...] + k
        vacc[...] = v if first else vacc[...] + v

    for load in loads[2:7]:
        load.wait()
    project(p, 0, 512, True)
    from_sibling(sbuf, 0)
    project(h * 2 + 1 - c, 0, 512)
    cos_table, sin_table = cos[...], sin[...]
    for i in range(2):
        from_opposite(sbuf, 0, i)
        project(2 * (1 - h) + c, i, 256)
    for i in range(2):
        forwarded(sbuf, 0, i)
        project(2 * (1 - h) + 1 - c, i, 256)

    lane = lax.broadcasted_iota(jnp.int32, (T, T), 1)
    key = rope(kacc[...], cos_table, sin_table)
    swapped = pltpu.roll(key, 64, 1)
    zero = jnp.zeros_like(key)
    low = lane < 64
    keys = [
        jnp.concatenate([jnp.where(low, key, zero), jnp.where(low, zero, swapped)], axis=0).astype(BF),
        jnp.concatenate([jnp.where(low, swapped, zero), jnp.where(low, zero, key)], axis=0).astype(BF),
    ]
    value_t = jnp.transpose(vacc[...]).astype(BF)
    row = lax.broadcasted_iota(jnp.int32, (T, T), 0)
    causal = row >= lane
    for j in range(4):
        query = rope(qacc[:, 128 * j : 128 * j + 128], cos_table, sin_table).astype(BF)
        scores = nt(query, keys[j // 2]) * HEAD_DIM ** (-0.5)
        for e in range(2):
            s = jnp.where(causal, scores[:, 128 * e : 128 * e + 128], -jnp.inf)
            s = jnp.exp(s - jnp.max(s, axis=1, keepdims=True))
            pst[2 * j + e] = (s / jnp.sum(s, axis=1, keepdims=True)).astype(BF)
    for g in range(2):
        probs = pst[4 * g : 4 * g + 4].reshape(4 * T, T)
        attended = nt(value_t[64 * g : 64 * g + 64], probs).astype(BF)
        for e in range(4):
            r = 64 * (4 * g + e)
            abuf[z, r : r + 64, :] = attended[:, 128 * e : 128 * e + 128]

    def along_z(buf, send, recv, k):
        push(buf.at[z], buf.at[z], send.at[k], recv.at[k], (z ^ k, x, y, h, c))

    inner = (z == 1) | (z == 2)
    outer = (z == 0) | (z == 3)
    second = jnp.where(inner, 3, 2)
    third = jnp.where(inner, 2, 3)

    def hand(slot, k, step):
        return remote(abuf.at[z ^ slot], abuf.at[z ^ slot], acs.at[step], acr.at[slot ^ k], (z ^ k, x, y, h, c))

    def attended_from(k):
        arrived(abuf.at[z ^ k], acs.at[0], acr.at[k])

    hand(0, 1, 0).start()

    @pl.when(inner)
    def _():
        hand(0, 3, 1).start()

    mine = pl.ds(pl.multiple_of(64 * c, 64), 64)
    others = pl.ds(pl.multiple_of(64 * (1 - c), 64), 64)

    def quarter(buf, kept, send, recv, i, dw):
        push(buf.at[(z + dw) % 4, mine, :], kept.at[z, mine, :], send.at[i], recv.at[i], in_column(dw, 0))

    def relay(kept, send, recv, k):
        i = 2 if k == 2 else (1 - z % 2 if k == 1 else z % 2)
        arrived(kept.at[z ^ k, mine, :], send.at[i], recv.at[i])
        push(kept.at[z ^ k, mine, :], kept.at[z ^ k, mine, :], send.at[2 + k], recv.at[2 + k], sibling)

    def complete(kept, send, recv, k):
        arrived(kept.at[z ^ k, others, :], send.at[2 + k], recv.at[2 + k])

    def own_quarter():
        return remote(cq.at[z, mine, :], cq.at[z, mine, :], ccs.at[4], ccr.at[4 + z], sibling)

    def relay_wo(k):
        zz = z ^ k
        arrived(cq.at[zz, mine, :], ccs.at[0], ccr.at[zz])
        push(cq.at[zz, mine, :], cq.at[zz, mine, :], ccs.at[4 + k], ccr.at[4 + zz], sibling)

    from_sibling(cbuf, 5)

    @pl.when(near)
    def _():
        cq[z] = cbuf[z]

    @pl.when(jnp.logical_not(near))
    def _():
        arrived(cq.at[z, mine, :], ccs.at[0], ccr.at[z])
        own_quarter().start()
        arrived(cq.at[z, others, :], ccs.at[0], ccr.at[4 + z])

    def rows_out(k, i, to, device):
        return remote(tsend.at[k, to, pl.ds(0, 128)], tbuf.at[z ^ k, plane, pl.ds(0, 128)], hs.at[k, i], hr.at[k, i], device)

    def tile_wo(k, right):
        for rb in range(4):
            block = nn(abuf[z ^ k, 128 * rb : 128 * rb + 128, :], right).astype(BF)
            for cb in range(4):
                tsend[k, rb * 4 + cb, 0:128, :] = block[:, 128 * cb : 128 * cb + 128]
        tbuf[z ^ k, plane, 0:128, :] = tsend[k, plane, 0:128, :]
        for i, (a, b) in enumerate(PLANE):
            to = (x + a) % 4 * 4 + (y + b) % 4
            rows_out(k, i, to, in_plane(a, b)).start()

    def tile_wv(k, right):
        block = nn(vbuf[z ^ k], right).astype(BF)
        for rb in range(4):
            for cb in range(4):
                tsend[k, rb * 4 + cb, 128:160, :] = block[32 * rb : 32 * rb + 32, 128 * cb : 128 * cb + 128]
        tbuf[z ^ k, plane, 128:160, :] = tsend[k, plane, 128:160, :]
        for i, (a, b) in enumerate(PLANE):
            to = (x + a) % 4 * 4 + (y + b) % 4
            push(tsend.at[k, to, pl.ds(128, 32)], tbuf.at[z ^ k, plane, pl.ds(128, 32)], gs.at[k, i], gr.at[k, i], in_plane(a, b))

    tile_wo(0, cq[z])
    gram_in[...] = jnp.zeros_like(gram_in)

    def settle_wo(k):
        def take(src, carry):
            gram_in[pl.ds((z ^ k) * 16 + src, 128, stride=PITCH), :] = tbuf[z ^ k, src, 0:128, :].astype(F32)
            return carry

        for i, (a, b) in enumerate(PLANE):
            src = (x - a) % 4 * 4 + (y - b) % 4
            arrived(tbuf.at[z ^ k, src, pl.ds(0, 128)], hs.at[k, i], hr.at[k, i])
        lax.fori_loop(0, 16, take, 0)

    def settle_wv(k):
        def take(src, carry):
            gram_in[pl.ds(128 * PITCH + (z ^ k) * 16 + src, 32, stride=PITCH), :] = tbuf[z ^ k, src, 128:160, :].astype(F32)
            return carry

        for i, (a, b) in enumerate(PLANE):
            src = (x - a) % 4 * 4 + (y - b) % 4
            arrived(tbuf.at[z ^ k, src, pl.ds(128, 32)], gs.at[k, i], gr.at[k, i])
        lax.fori_loop(0, 16, take, 0)

    def next_wo(k):
        zz = z ^ k
        arrived(cq.at[zz, others, :], ccs.at[0], ccr.at[4 + zz])
        tile_wo(k, cq[zz])

    def next_wv(k):
        arrived(vbuf.at[z ^ k], vcs.at[k], vcr.at[k])
        complete(sq, scs, scr, k)
        tile_wv(k, sq[z ^ k])

    attended_from(1)

    @pl.when(inner)
    def _():
        hand(1, 3, 2).start()
        attended_from(3)
        hand(3, 1, 3).start()

    @pl.when(p != z)
    def _():
        cot_half(p, 0, 5, opposite).start()

    relay_wo(1)
    next_wo(1)
    relay_wo(3)
    relay_wo(2)

    @pl.when(inner)
    def _():
        attended_from(2)
        hand(2, 1, 4).start()

    @pl.when(outer)
    def _():
        attended_from(2)

    @pl.when(p != z)
    def _():
        cot_half(p, 1, 5, opposite).start()

    next_wo(second)
    @pl.when(outer)
    def _():
        attended_from(3)

    next_wo(third)

    def grad_part(part):
        cols = pl.ds(pl.multiple_of(part * 512, 512), 512)
        return nt(wob[:, cols], cbuf[part])

    loads[7].wait()
    gacc[...] = grad_part(p) + grad_part(h * 2 + 1 - c)

    @pl.when(jnp.logical_not(kept_here))
    def _():
        for i in range(2):
            cot_half(2 * (1 - h) + c, i, 5, opposite).wait_recv()
            cot_half(2 * (1 - h) + c, i, 8, sibling).start()

    @pl.when(kept_here)
    def _():
        cbuf[2 * (1 - h) + c] = cq[z]

    quarter(sbuf, sq, scs, scr, 0, 1)
    quarter(sbuf, sq, scs, scr, 1, 7)
    quarter(sbuf, sq, scs, scr, 2, 2)
    gacc[...] = gacc[...] + grad_part(2 * (1 - h) + c)

    @pl.when(jnp.logical_not(kept_there))
    def _():
        for i in range(2):
            cot_half(2 * (1 - h) + 1 - c, i, 8, sibling).wait_recv()

    @pl.when(kept_there)
    def _():
        cbuf[2 * (1 - h) + 1 - c] = cq[z]

    gacc[...] = gacc[...] + grad_part(2 * (1 - h) + 1 - c)
    for g in range(2):
        left = jnp.concatenate([gacc[64 * (4 * g + e) : 64 * (4 * g + e) + 64, :] for e in range(4)], axis=1).astype(BF)
        vbuf[z, 64 * g : 64 * g + 64, :] = nn(left, pst[4 * g : 4 * g + 4].reshape(4 * T, T)).astype(BF)
    along_z(vbuf, vcs, vcr, 1)
    along_z(vbuf, vcs, vcr, 3)
    along_z(vbuf, vcs, vcr, 2)
    tile_wv(0, sbuf[z])
    relay(sq, scs, scr, 1)
    relay(sq, scs, scr, 3)
    relay(sq, scs, scr, 2)
    for k in (1, 3, 2):
        next_wv(k)

    def pair(r, u, first, size):
        at = (r * 32 + 2 * u) * PITCH + first
        upper = gram_in[pl.ds(pl.multiple_of(at, 8), size), :]
        lower = gram_in[pl.ds(pl.multiple_of(at + PITCH, 8), size), :]
        return jnp.concatenate([upper, lower], axis=1).astype(BF)

    def products(r, total):
        for u in range(16):
            both = pair(r, u, 0, 64)
            total = total + nt(both, both)
        return total

    late = (z ^ third) * 16

    def late_products(r, total):
        for u in range(16):
            total = total + nt(pair(r, u, 0, 64), pair(r, u, late, 16))
        return total

    for k in (0, 1, second):
        settle_wo(k)
    kd[:, 0:64] = lax.fori_loop(0, 4, products, jnp.zeros((64, 64), F32))
    settle_wv(0)
    settle_wv(1)
    settle_wo(third)
    strip = lax.fori_loop(0, 4, late_products, jnp.zeros((64, 16), F32))
    wide = jnp.concatenate([strip, jnp.zeros((64, 112), F32)], axis=1)
    wide = pltpu.roll(wide, late, 1)[:, 0:64]
    lanes = lax.broadcasted_iota(jnp.int32, (64, 64), 1)
    kd[:, 0:64] = jnp.where((lanes >= late) & (lanes < late + 16), wide, kd[:, 0:64])
    kd[pl.ds(pl.multiple_of(late, 16), 16), 0:64] = jnp.transpose(strip)
    settle_wv(3)
    settle_wv(2)
    kd[:, 0:64] = products(4, kd[:, 0:64])
    eye = lax.broadcasted_iota(jnp.int32, (64, 64), 0) == lanes
    diag = jnp.sum(jnp.where(eye, kd[:, 0:64], 0.0), axis=0, keepdims=True)
    kd[:, 64:128] = jnp.broadcast_to(diag, (64, 64))
    for g in range(16):
        fin[g] = kd[pl.ds(g, 4, stride=16), :]
    f1[plane] = fin[plane]
    for i, (a, b) in enumerate(PLANE):
        to = (x + a) % 4 * 4 + (y + b) % 4
        push(fin.at[to], f1.at[plane], f1s.at[i], f1r.at[i], in_plane(a, b))
    for i, (a, b) in enumerate(PLANE):
        src = (x - a) % 4 * 4 + (y - b) % 4
        arrived(f1.at[src], f1s.at[i], f1r.at[i])
    rows = jnp.sum(f1[...], axis=0)
    for zz in range(4):
        rowbuf[zz] = rows[zz : zz + 1]
    f2[column] = rowbuf[z]
    for i, (dw, dc) in enumerate(COLUMN):
        to = in_column(dw, dc)
        push(rowbuf.at[to[0]], f2.at[column], f2s.at[i], f2r.at[i], to)
    for i, (dw, dc) in enumerate(COLUMN):
        src = (w - dw) % 8 * 2 + (c - dc) % 2
        arrived(f2.at[src], f2s.at[i], f2r.at[i])
    total = jnp.sum(f2[...], axis=0)
    entries, diagonal = total[:, 0:64], total[:, 64:128]
    own_lane = lax.broadcasted_iota(jnp.int32, (1, 64), 1) == z * 16 + plane
    own = jnp.sum(jnp.where(own_lane, diagonal, 0.0), axis=1, keepdims=True)
    out[...] = entries / jnp.sqrt(own * diagonal)
    for copy in sent:
        copy.wait_send()
    for k in range(4):
        for i, (a, b) in enumerate(PLANE):
            rows_out(k, i, 0, in_plane(a, b)).wait_send()

    @pl.when(p != z)
    def _():
        for i in range(2):
            cot_half(p, i, 5, opposite).wait_send()

    @pl.when(jnp.logical_not(kept_here))
    def _():
        for i in range(2):
            cot_half(p, i, 8, sibling).wait_send()

    hand(0, 1, 0).wait_send()
    for core in range(2):
        spread(1 - h, 0, core).wait_send()

    @pl.when(z != p)
    def _():
        for core in range(2):
            spread(h, 1, core).wait_send()

    @pl.when(jnp.logical_not(near))
    def _():
        own_quarter().wait_send()

    @pl.when(inner)
    def _():
        for step in range(1, 5):
            hand(0, 1, step).wait_send()


def on_device(states, cotangent, wq, wk, wv, wo):
    cos, sin = rope_tables()
    any_spec = pl.BlockSpec(memory_space=pl.ANY)
    dma = pltpu.SemaphoreType.DMA
    shapes = [
        ((2048, 512), BF), ((2048, 128), BF), ((2048, 128), BF), ((512, 2048), BF), ((T, T), F32), ((T, T), F32),
        ((4, T, 512), BF), ((4, T, 512), BF), ((4, T, 512), BF), ((4, T, 512), BF),
        ((T, 512), F32), ((T, 128), F32), ((T, 128), F32), ((512, T), F32),
        ((8, T, T), BF), ((4, 512, T), BF), ((4, 128, T), BF),
        ((4, 16, 160, 128), BF), ((4, 16, 160, 128), BF),
        ((160 * PITCH, 128), F32), ((64, 128), F32), ((16, 4, 128), F32), ((16, 4, 128), F32),
        ((4, 1, 128), F32), ((16, 1, 128), F32),
    ]
    sems = [(8,)] + [(10,)] * 2 + [(5,)] * 4 + [(8,)] * 4 + [(4, 15)] * 4 + [(15,)] * 4
    return pl.pallas_call(
        kernel,
        out_shape=jax.ShapeDtypeStruct((1, 64), F32),
        in_specs=[any_spec] * 8,
        out_specs=pl.BlockSpec(memory_space=pltpu.VMEM),
        scratch_shapes=[pltpu.VMEM(s, t) for s, t in shapes] + [dma(s) for s in sems],
        compiler_params=pltpu.CompilerParams(
            collective_id=0, has_side_effects=True, vmem_limit_bytes=60 * 2**20),
        name="ntk_gram",
    )(states, cotangent, wq, wk, wv, wo, jnp.asarray(cos), jnp.asarray(sin))


def solution(mesh):
    split = Mesh(mesh.devices.reshape(4, 4, 4, 2, 2), AXES)
    seq, tp = ("z", "x", "y"), ("h", "c")
    return jax.shard_map(
        on_device,
        mesh=split,
        in_specs=(P(seq, None, tp), P(seq, None, tp), P(None, tp), P(None, tp), P(None, tp), P(tp, None)),
        out_specs=P(seq, None),
        check_vma=False,
    )
```

```python
import functools

import jax
import jax.numpy as jnp
import numpy as np
from jax import lax
from jax.experimental import pallas as pl
from jax.experimental.pallas import tpu as pltpu
from jax.sharding import Mesh
from jax.sharding import PartitionSpec as P

AXES = ("z", "x", "y", "h", "c")
MESH = pl.DeviceIdType.MESH
HEAD_DIM = 64
THETA = 500000.0
T = 128
PITCH = 72
BF = jnp.bfloat16
F32 = jnp.float32

PLANE = [(2, 2), (2, 1), (1, 2), (2, 3), (3, 2), (1, 1), (3, 3), (1, 3), (3, 1), (2, 0), (0, 2), (1, 0), (3, 0), (0, 1), (0, 3)]
COLUMN = [(w, c) for w in range(8) for c in range(2) if (w, c) != (0, 0)]


def nn(a, b):
    return lax.dot_general(a, b, (((1,), (0,)), ((), ())), preferred_element_type=F32)


def nt(a, b):
    return lax.dot_general(a, b, (((1,), (1,)), ((), ())), preferred_element_type=F32)


def rope_tables():
    k = np.arange(HEAD_DIM // 2, dtype=np.float64)
    freq = THETA ** (-2.0 * k / HEAD_DIM)
    angle = np.arange(T, dtype=np.float64)[:, None] * freq[None, :]
    cos, sin = np.cos(angle), np.sin(angle)
    cos = np.concatenate([cos, cos] * 2, axis=1)
    sin = np.concatenate([-sin, sin] * 2, axis=1)
    return cos.astype(np.float32), sin.astype(np.float32)


def rope(v, cos, sin):
    lane = lax.broadcasted_iota(jnp.int32, v.shape, 1)
    turned = jnp.where(lane % 64 < 32, pltpu.roll(v, 96, 1), pltpu.roll(v, 32, 1))
    return v * cos + turned * sin


def kernel(st, ct, wq, wk, wv, wo, cos_in, sin_in, out, wqb, wkb, wvb, wob, cos, sin, sbuf, cbuf, sq, cq, qacc, kacc, vacc, gacc,
           pst, abuf, vbuf, tsend, tbuf, gram_in, kd, fin, f1, rowbuf, f2,
           loc, tps, tpr, acs, acr, vcs, vcr, ccs, ccr, scs, scr, hs, hr, gs, gr, f1s, f1r, f2s, f2r):
    z, x, y, h, c = [lax.axis_index(a) for a in AXES]
    w = h * 4 + z
    p = h * 2 + c
    plane = x * 4 + y
    column = w * 2 + c

    def in_plane(a, b):
        return (z, (x + a) % 4, (y + b) % 4, h, c)

    def in_column(dw, dc):
        v = (w + dw) % 8
        return (v % 4, x, y, v // 4, (c + dc) % 2)

    sibling = in_column(0, 1)
    opposite = in_column(4, 0)

    def remote(src, dst, send, recv, device):
        return pltpu.make_async_remote_copy(
            src_ref=src, dst_ref=dst, send_sem=send, recv_sem=recv, device_id=device, device_id_type=MESH)

    sent = []

    def push(src, dst, send, recv, device):
        copy = remote(src, dst, send, recv, device)
        copy.start()
        sent.append(copy)

    def arrived(slot, send, recv):
        remote(slot, slot, send, recv, sibling).wait_recv()

    barrier = pltpu.get_barrier_semaphore()
    for dw, dc in COLUMN:
        pl.semaphore_signal(barrier, inc=1, device_id=in_column(dw, dc), device_id_type=MESH)
    for a, b in PLANE:
        pl.semaphore_signal(barrier, inc=1, device_id=in_plane(a, b), device_id_type=MESH)
    loads = [pltpu.make_async_copy(a, b, loc.at[i]) for i, (a, b) in enumerate(
        [(st.at[0], sbuf.at[p]), (ct.at[0], cbuf.at[p]), (wq, wqb), (wk, wkb), (wv, wvb), (cos_in, cos), (sin_in, sin), (wo, wob)])]
    for load in loads:
        load.start()
    pl.semaphore_wait(barrier, len(PLANE) + len(COLUMN))

    halves = [pl.ds(0, 256), pl.ds(256, 256)]

    def to_opposite(buf, base):
        for i, cols in enumerate(halves):
            push(buf.at[p, :, cols], buf.at[p, :, cols], tps.at[base + i], tpr.at[base + i], opposite)

    def to_sibling(buf, base):
        push(buf.at[p], buf.at[p], tps.at[base + 2], tpr.at[base + 2], sibling)

    near = (h == z // 2)
    strips = [pl.ds(0, 64), pl.ds(64, 64)]

    def spread(t, which, core):
        rows = strips[core]
        return remote(cbuf.at[p, rows, :], cq.at[z, rows, :], ccs.at[2 * which + core], ccr.at[z], (p, x, y, t, core))

    kept_here = 2 * (1 - h) + c == z
    kept_there = 2 * (1 - h) + 1 - c == z

    def cot_half(part, i, at, device):
        cols = halves[i]
        return remote(cbuf.at[part, :, cols], cbuf.at[part, :, cols], tps.at[at + i], tpr.at[at + i], device)

    def from_sibling(buf, base):
        arrived(buf.at[h * 2 + 1 - c], tps.at[base + 2], tpr.at[base + 2])

    def from_opposite(buf, base, i):
        part = buf.at[2 * (1 - h) + c, :, halves[i]]
        arrived(part, tps.at[base + i], tpr.at[base + i])
        push(part, part, tps.at[base + 3 + i], tpr.at[base + 3 + i], sibling)

    def forwarded(buf, base, i):
        arrived(buf.at[2 * (1 - h) + 1 - c, :, halves[i]], tps.at[base + 3 + i], tpr.at[base + 3 + i])

    loads[0].wait()
    to_opposite(sbuf, 0)
    to_sibling(sbuf, 0)
    loads[1].wait()
    to_sibling(cbuf, 5)
    for core in range(2):
        spread(1 - h, 0, core).start()

    @pl.when(z != p)
    def _():
        for core in range(2):
            spread(h, 1, core).start()

    def project(part, i, width, first=False):
        rows = pl.ds(pl.multiple_of(part * 512 + 256 * i, 256), width)
        s = sbuf[part, :, 256 * i : 256 * i + width]
        q, k, v = nn(s, wqb[rows, :]), nn(s, wkb[rows, :]), nn(s, wvb[rows, :])
        qacc[...] = q if first else qacc[...] + q
        kacc[...] = k if first else kacc[...] + k
        vacc[...] = v if first else vacc[...] + v

    for load in loads[2:7]:
        load.wait()
    project(p, 0, 512, True)
    from_sibling(sbuf, 0)
    project(h * 2 + 1 - c, 0, 512)
    cos_table, sin_table = cos[...], sin[...]
    for i in range(2):
        from_opposite(sbuf, 0, i)
        project(2 * (1 - h) + c, i, 256)
    for i in range(2):
        forwarded(sbuf, 0, i)
        project(2 * (1 - h) + 1 - c, i, 256)

    lane = lax.broadcasted_iota(jnp.int32, (T, T), 1)
    key = rope(kacc[...], cos_table, sin_table)
    swapped = pltpu.roll(key, 64, 1)
    zero = jnp.zeros_like(key)
    low = lane < 64
    keys = [
        jnp.concatenate([jnp.where(low, key, zero), jnp.where(low, zero, swapped)], axis=0).astype(BF),
        jnp.concatenate([jnp.where(low, swapped, zero), jnp.where(low, zero, key)], axis=0).astype(BF),
    ]
    value_t = jnp.transpose(vacc[...]).astype(BF)
    row = lax.broadcasted_iota(jnp.int32, (T, T), 0)
    causal = row >= lane
    for j in range(4):
        query = rope(qacc[:, 128 * j : 128 * j + 128], cos_table, sin_table).astype(BF)
        scores = nt(query, keys[j // 2]) * HEAD_DIM ** (-0.5)
        for e in range(2):
            s = jnp.where(causal, scores[:, 128 * e : 128 * e + 128], -jnp.inf)
            s = jnp.exp(s - jnp.max(s, axis=1, keepdims=True))
            pst[2 * j + e] = (s / jnp.sum(s, axis=1, keepdims=True)).astype(BF)
    for g in range(2):
        probs = pst[4 * g : 4 * g + 4].reshape(4 * T, T)
        attended = nt(value_t[64 * g : 64 * g + 64], probs).astype(BF)
        for e in range(4):
            r = 64 * (4 * g + e)
            abuf[z, r : r + 64, :] = attended[:, 128 * e : 128 * e + 128]

    def along_z(buf, send, recv, k):
        push(buf.at[z], buf.at[z], send.at[k], recv.at[k], (z ^ k, x, y, h, c))

    inner = (z == 1) | (z == 2)
    outer = (z == 0) | (z == 3)
    second = jnp.where(inner, 3, 2)
    third = jnp.where(inner, 2, 3)

    def hand(slot, k, step):
        return remote(abuf.at[z ^ slot], abuf.at[z ^ slot], acs.at[step], acr.at[slot ^ k], (z ^ k, x, y, h, c))

    def attended_from(k):
        arrived(abuf.at[z ^ k], acs.at[0], acr.at[k])

    hand(0, 1, 0).start()

    @pl.when(inner)
    def _():
        hand(0, 3, 1).start()

    mine = pl.ds(pl.multiple_of(64 * c, 64), 64)
    others = pl.ds(pl.multiple_of(64 * (1 - c), 64), 64)

    def quarter(buf, kept, send, recv, i, dw):
        push(buf.at[(z + dw) % 4, mine, :], kept.at[z, mine, :], send.at[i], recv.at[i], in_column(dw, 0))

    def relay(kept, send, recv, k):
        i = 2 if k == 2 else (1 - z % 2 if k == 1 else z % 2)
        arrived(kept.at[z ^ k, mine, :], send.at[i], recv.at[i])
        push(kept.at[z ^ k, mine, :], kept.at[z ^ k, mine, :], send.at[2 + k], recv.at[2 + k], sibling)

    def complete(kept, send, recv, k):
        arrived(kept.at[z ^ k, others, :], send.at[2 + k], recv.at[2 + k])

    def own_quarter():
        return remote(cq.at[z, mine, :], cq.at[z, mine, :], ccs.at[4], ccr.at[4 + z], sibling)

    def relay_wo(k):
        zz = z ^ k
        arrived(cq.at[zz, mine, :], ccs.at[0], ccr.at[zz])
        push(cq.at[zz, mine, :], cq.at[zz, mine, :], ccs.at[4 + k], ccr.at[4 + zz], sibling)

    from_sibling(cbuf, 5)

    @pl.when(near)
    def _():
        cq[z] = cbuf[z]

    @pl.when(jnp.logical_not(near))
    def _():
        arrived(cq.at[z, mine, :], ccs.at[0], ccr.at[z])
        own_quarter().start()
        arrived(cq.at[z, others, :], ccs.at[0], ccr.at[4 + z])

    def rows_out(k, i, to, device):
        return remote(tsend.at[k, to, pl.ds(0, 128)], tbuf.at[z ^ k, plane, pl.ds(0, 128)], hs.at[k, i], hr.at[k, i], device)

    def tile_wo(k, right):
        for rb in range(4):
            block = nn(abuf[z ^ k, 128 * rb : 128 * rb + 128, :], right).astype(BF)
            for cb in range(4):
                tsend[k, rb * 4 + cb, 0:128, :] = block[:, 128 * cb : 128 * cb + 128]
        tbuf[z ^ k, plane, 0:128, :] = tsend[k, plane, 0:128, :]
        for i, (a, b) in enumerate(PLANE):
            to = (x + a) % 4 * 4 + (y + b) % 4
            rows_out(k, i, to, in_plane(a, b)).start()

    def tile_wv(k, right):
        block = nn(vbuf[z ^ k], right).astype(BF)
        for rb in range(4):
            for cb in range(4):
                tsend[k, rb * 4 + cb, 128:160, :] = block[32 * rb : 32 * rb + 32, 128 * cb : 128 * cb + 128]
        tbuf[z ^ k, plane, 128:160, :] = tsend[k, plane, 128:160, :]
        for i, (a, b) in enumerate(PLANE):
            to = (x + a) % 4 * 4 + (y + b) % 4
            push(tsend.at[k, to, pl.ds(128, 32)], tbuf.at[z ^ k, plane, pl.ds(128, 32)], gs.at[k, i], gr.at[k, i], in_plane(a, b))

    tile_wo(0, cq[z])
    gram_in[...] = jnp.zeros_like(gram_in)

    def settle_wo(k):
        def take(src, carry):
            gram_in[pl.ds((z ^ k) * 16 + src, 128, stride=PITCH), :] = tbuf[z ^ k, src, 0:128, :].astype(F32)
            return carry

        for i, (a, b) in enumerate(PLANE):
            src = (x - a) % 4 * 4 + (y - b) % 4
            arrived(tbuf.at[z ^ k, src, pl.ds(0, 128)], hs.at[k, i], hr.at[k, i])
        lax.fori_loop(0, 16, take, 0)

    def settle_wv(k):
        def take(src, carry):
            gram_in[pl.ds(128 * PITCH + (z ^ k) * 16 + src, 32, stride=PITCH), :] = tbuf[z ^ k, src, 128:160, :].astype(F32)
            return carry

        for i, (a, b) in enumerate(PLANE):
            src = (x - a) % 4 * 4 + (y - b) % 4
            arrived(tbuf.at[z ^ k, src, pl.ds(128, 32)], gs.at[k, i], gr.at[k, i])
        lax.fori_loop(0, 16, take, 0)

    def next_wo(k):
        zz = z ^ k
        arrived(cq.at[zz, others, :], ccs.at[0], ccr.at[4 + zz])
        tile_wo(k, cq[zz])

    def next_wv(k):
        arrived(vbuf.at[z ^ k], vcs.at[k], vcr.at[k])
        complete(sq, scs, scr, k)
        tile_wv(k, sq[z ^ k])

    attended_from(1)

    @pl.when(inner)
    def _():
        hand(1, 3, 2).start()
        attended_from(3)
        hand(3, 1, 3).start()

    @pl.when(p != z)
    def _():
        cot_half(p, 0, 5, opposite).start()

    relay_wo(1)
    next_wo(1)
    relay_wo(3)
    relay_wo(2)

    @pl.when(inner)
    def _():
        attended_from(2)
        hand(2, 1, 4).start()

    @pl.when(outer)
    def _():
        attended_from(2)

    @pl.when(p != z)
    def _():
        cot_half(p, 1, 5, opposite).start()

    next_wo(second)
    @pl.when(outer)
    def _():
        attended_from(3)

    next_wo(third)

    def grad_part(part):
        cols = pl.ds(pl.multiple_of(part * 512, 512), 512)
        return nt(wob[:, cols], cbuf[part])

    loads[7].wait()
    gacc[...] = grad_part(p) + grad_part(h * 2 + 1 - c)

    @pl.when(jnp.logical_not(kept_here))
    def _():
        for i in range(2):
            cot_half(2 * (1 - h) + c, i, 5, opposite).wait_recv()
            cot_half(2 * (1 - h) + c, i, 8, sibling).start()

    @pl.when(kept_here)
    def _():
        cbuf[2 * (1 - h) + c] = cq[z]

    quarter(sbuf, sq, scs, scr, 0, 1)
    quarter(sbuf, sq, scs, scr, 1, 7)
    quarter(sbuf, sq, scs, scr, 2, 2)
    gacc[...] = gacc[...] + grad_part(2 * (1 - h) + c)

    @pl.when(jnp.logical_not(kept_there))
    def _():
        for i in range(2):
            cot_half(2 * (1 - h) + 1 - c, i, 8, sibling).wait_recv()

    @pl.when(kept_there)
    def _():
        cbuf[2 * (1 - h) + 1 - c] = cq[z]

    gacc[...] = gacc[...] + grad_part(2 * (1 - h) + 1 - c)
    for g in range(2):
        left = jnp.concatenate([gacc[64 * (4 * g + e) : 64 * (4 * g + e) + 64, :] for e in range(4)], axis=1).astype(BF)
        vbuf[z, 64 * g : 64 * g + 64, :] = nn(left, pst[4 * g : 4 * g + 4].reshape(4 * T, T)).astype(BF)
    along_z(vbuf, vcs, vcr, 1)
    along_z(vbuf, vcs, vcr, 3)
    along_z(vbuf, vcs, vcr, 2)
    tile_wv(0, sbuf[z])
    relay(sq, scs, scr, 1)
    relay(sq, scs, scr, 3)
    relay(sq, scs, scr, 2)
    for k in (1, 3, 2):
        next_wv(k)

    def pair(r, u, first, size):
        at = (r * 32 + 2 * u) * PITCH + first
        upper = gram_in[pl.ds(pl.multiple_of(at, 8), size), :]
        lower = gram_in[pl.ds(pl.multiple_of(at + PITCH, 8), size), :]
        return jnp.concatenate([upper, lower], axis=1).astype(BF)

    def products(r, total):
        for u in range(16):
            both = pair(r, u, 0, 64)
            total = total + nt(both, both)
        return total

    late = (z ^ third) * 16

    def late_products(r, total):
        for u in range(16):
            total = total + nt(pair(r, u, 0, 64), pair(r, u, late, 16))
        return total

    for k in (0, 1, second):
        settle_wo(k)
    kd[:, 0:64] = lax.fori_loop(0, 4, products, jnp.zeros((64, 64), F32))
    settle_wv(0)
    settle_wv(1)
    settle_wo(third)
    strip = lax.fori_loop(0, 4, late_products, jnp.zeros((64, 16), F32))
    wide = jnp.concatenate([strip, jnp.zeros((64, 112), F32)], axis=1)
    wide = pltpu.roll(wide, late, 1)[:, 0:64]
    lanes = lax.broadcasted_iota(jnp.int32, (64, 64), 1)
    kd[:, 0:64] = jnp.where((lanes >= late) & (lanes < late + 16), wide, kd[:, 0:64])
    kd[pl.ds(pl.multiple_of(late, 16), 16), 0:64] = jnp.transpose(strip)
    settle_wv(3)
    settle_wv(2)
    kd[:, 0:64] = products(4, kd[:, 0:64])
    eye = lax.broadcasted_iota(jnp.int32, (64, 64), 0) == lanes
    diag = jnp.sum(jnp.where(eye, kd[:, 0:64], 0.0), axis=0, keepdims=True)
    kd[:, 64:128] = jnp.broadcast_to(diag, (64, 64))
    for g in range(16):
        fin[g] = kd[pl.ds(g, 4, stride=16), :]
    f1[plane] = fin[plane]
    for i, (a, b) in enumerate(PLANE):
        to = (x + a) % 4 * 4 + (y + b) % 4
        push(fin.at[to], f1.at[plane], f1s.at[i], f1r.at[i], in_plane(a, b))
    for i, (a, b) in enumerate(PLANE):
        src = (x - a) % 4 * 4 + (y - b) % 4
        arrived(f1.at[src], f1s.at[i], f1r.at[i])
    rows = jnp.sum(f1[...], axis=0)
    for zz in range(4):
        rowbuf[zz] = rows[zz : zz + 1]
    f2[column] = rowbuf[z]
    for i, (dw, dc) in enumerate(COLUMN):
        to = in_column(dw, dc)
        push(rowbuf.at[to[0]], f2.at[column], f2s.at[i], f2r.at[i], to)
    for i, (dw, dc) in enumerate(COLUMN):
        src = (w - dw) % 8 * 2 + (c - dc) % 2
        arrived(f2.at[src], f2s.at[i], f2r.at[i])
    total = jnp.sum(f2[...], axis=0)
    entries, diagonal = total[:, 0:64], total[:, 64:128]
    own_lane = lax.broadcasted_iota(jnp.int32, (1, 64), 1) == z * 16 + plane
    own = jnp.sum(jnp.where(own_lane, diagonal, 0.0), axis=1, keepdims=True)
    out[0:1, :] = entries
    out[1:2, :] = own * diagonal
    for copy in sent:
        copy.wait_send()
    for k in range(4):
        for i, (a, b) in enumerate(PLANE):
            rows_out(k, i, 0, in_plane(a, b)).wait_send()

    @pl.when(p != z)
    def _():
        for i in range(2):
            cot_half(p, i, 5, opposite).wait_send()

    @pl.when(jnp.logical_not(kept_here))
    def _():
        for i in range(2):
            cot_half(p, i, 8, sibling).wait_send()

    hand(0, 1, 0).wait_send()
    for core in range(2):
        spread(1 - h, 0, core).wait_send()

    @pl.when(z != p)
    def _():
        for core in range(2):
            spread(h, 1, core).wait_send()

    @pl.when(jnp.logical_not(near))
    def _():
        own_quarter().wait_send()

    @pl.when(inner)
    def _():
        for step in range(1, 5):
            hand(0, 1, step).wait_send()


def on_device(states, cotangent, wq, wk, wv, wo):
    cos, sin = rope_tables()
    any_spec = pl.BlockSpec(memory_space=pl.ANY)
    dma = pltpu.SemaphoreType.DMA
    shapes = [
        ((2048, 512), BF), ((2048, 128), BF), ((2048, 128), BF), ((512, 2048), BF), ((T, T), F32), ((T, T), F32),
        ((4, T, 512), BF), ((4, T, 512), BF), ((4, T, 512), BF), ((4, T, 512), BF),
        ((T, 512), F32), ((T, 128), F32), ((T, 128), F32), ((512, T), F32),
        ((8, T, T), BF), ((4, 512, T), BF), ((4, 128, T), BF),
        ((4, 16, 160, 128), BF), ((4, 16, 160, 128), BF),
        ((160 * PITCH, 128), F32), ((64, 128), F32), ((16, 4, 128), F32), ((16, 4, 128), F32),
        ((4, 1, 128), F32), ((16, 1, 128), F32),
    ]
    sems = [(8,)] + [(10,)] * 2 + [(5,)] * 4 + [(8,)] * 4 + [(4, 15)] * 4 + [(15,)] * 4
    both = pl.pallas_call(
        kernel,
        out_shape=jax.ShapeDtypeStruct((2, 64), F32),
        in_specs=[any_spec] * 8,
        out_specs=pl.BlockSpec(memory_space=pltpu.VMEM),
        scratch_shapes=[pltpu.VMEM(s, t) for s, t in shapes] + [dma(s) for s in sems],
        compiler_params=pltpu.CompilerParams(
            collective_id=0, has_side_effects=True, vmem_limit_bytes=60 * 2**20),
        name="ntk_gram",
    )(states, cotangent, wq, wk, wv, wo, jnp.asarray(cos), jnp.asarray(sin))
    return both[0:1] / jnp.sqrt(both[1:2])


def solution(mesh):
    split = Mesh(mesh.devices.reshape(4, 4, 4, 2, 2), AXES)
    seq, tp = ("z", "x", "y"), ("h", "c")
    return jax.shard_map(
        on_device,
        mesh=split,
        in_specs=(P(seq, None, tp), P(seq, None, tp), P(None, tp), P(None, tp), P(None, tp), P(tp, None)),
        out_specs=P(seq, None),
        check_vma=False,
    )
```
